32 devices in a mesh: rot: 8 (over z, y), cls: 4 (over x, core).
Axes of the slice: x: 2, y: 2, z: 4, core: 2. Of those that a mesh axis runs over, the one named last changes fastest.
Arguments:
- particles: bfloat16 [128, 16384], P('rot'), may hold values from -64 to 64
- references: bfloat16 [48, 96, 16384], P('cls', 'rot'), may hold values from -0.046875 to 0.046875
- micrograph: int32 [8, 16], P('rot'), may hold values from 0 to 3, never falling along the last dimension, each value on 1 to 8 neighbouring positions
- ctf: float32 [32, 64], P('rot'), may hold values from -1 to 1
- prior_class: int32 [128], P('rot'), may hold values from 0 to 47
Outputs:
- class_scores: float32 [128, 48], P('rot', 'cls')
- best_score: float32 [128], P('rot')
- prior_score: float32 [128], P('rot')
The draws below stay inside these ranges and needn't reach their ends.
Inputs may be any that keep to these rules, and one draw needn't show every extreme that they name: The entries of one row are the micrograph numbers of that index of rot in order, never falling; each of the 4 micrographs has 1 to 8 particles.
All inputs are finite; a program needn't handle non-finite values.
Results may differ from the reference program's by a relative error of at most 0.00095.
Values may be sent and summed in bfloat16 or wider, within the bound.
A program may use at most 128 MiB of HBM per device.

```python
import math
import jax
import jax.numpy as jnp
import numpy as np
from jax import lax

CYCLES = 64
POLAR = 128
F = 16384
CLASSES = 48
ANGLES = 96
PART_DEV = 16
MICS_DEV = 4
MOST = 8
PARTICLES = 128
MICS = 32
N_ROT = 8


def draw_particles(key, part):
    first, second = jax.random.split(key, 2)
    base = jnp.clip(jax.random.normal(first, (PARTICLES, CYCLES, 2 * POLAR), jnp.float32), -6.0, 6.0)
    level = jnp.exp(jax.random.uniform(second, (PARTICLES, CYCLES, 1), jnp.float32, 0.0, math.log(10.0)))
    values = base * level
    values = jnp.clip(values, -64.0, 64.0)
    return values.reshape(PARTICLES, F).astype(jnp.bfloat16)


def place_ends(entries, own_key, smallest, top_value):
    extent = entries.shape
    place = [jax.random.randint(jax.random.fold_in(own_key, axis), (), 0, extent[axis]) for axis in range(len(extent))]
    entries = entries.at[tuple(place)].set(smallest)
    longest = extent.index(max(extent))
    place[longest] = (place[longest] + 1) % extent[longest]
    return entries.at[tuple(place)].set(top_value)


def levels(key, extent, cuts, low, top_value):
    level, own = 1.0, jax.random.fold_in(key, 6)
    for position, shards_of in cuts:
        steps = jnp.exp(jax.random.uniform(jax.random.fold_in(own, position), (shards_of,), jnp.float32, low / len(cuts), top_value / len(cuts)))
        level = level * jnp.repeat(steps, extent[position] // shards_of).reshape([-1 if axis == position else 1 for axis in range(len(extent))])
    return level


def split_up(count, total, limit, lean):
    portions = [(1 << 20) // math.isqrt(rank ** lean) + 1 for rank in range(2, count + 1)]
    surplus, given = total - limit - (count - 1), [1] * (count - 1)
    while surplus > 0:
        candidates = [i for i in range(count - 1) if given[i] < limit]
        mass, budget = sum([portions[i] for i in candidates]), surplus
        for i in candidates:
            addition = min(limit - given[i], max(1, budget * portions[i] // mass), surplus)
            given[i] = given[i] + addition
            surplus = surplus - addition
    return np.array([limit] + given)


def uneven(stream_key, amount, total, limit, slope):
    if amount == 2:
        one = jax.random.randint(stream_key, (), max(1, total - limit), min(limit, total - 1) + 1)
        return jnp.stack([one, total - one])
    sizes = jnp.asarray(split_up(amount, total, limit, slope), jnp.int32)
    pairs = (amount - 1) // 2
    donor, receiver = sizes[1:1 + 2 * pairs:2], sizes[2:2 + 2 * pairs:2]
    margin = jnp.minimum(donor - 1, limit - receiver)
    passed = jax.random.randint(jax.random.fold_in(stream_key, 1), (pairs,), 0, 1 << 20) % (margin + 1)
    sizes = sizes.at[1:1 + 2 * pairs:2].set(donor - passed).at[2:2 + 2 * pairs:2].set(receiver + passed)
    return sizes[jax.random.permutation(jax.random.fold_in(stream_key, 2), amount)]


def normal_values(stream_key, extent, deviation, reach, pieces=(), kind=jnp.bfloat16):
    loudness = levels(stream_key, extent, pieces, -0.22, 0.18) if pieces else 1.0
    drawn = jax.random.normal(stream_key, extent, jnp.float32) * deviation * loudness
    return jnp.minimum(jnp.maximum(drawn, -reach), reach).astype(kind)


def setup_inputs(seed: int = 0) -> dict:
    streams_of = jax.random.split(jax.random.key(seed), 6)
    particles = draw_particles(jax.random.fold_in(streams_of[5], 71), 0)
    references = normal_values(streams_of[1], (CLASSES, ANGLES, F), F ** -0.5, 0.046875, ((0, 4), (1, 8)))
    micrograph = jax.vmap(lambda own: jnp.searchsorted(jnp.cumsum(uneven(own, MICS_DEV, PART_DEV, MOST, 2)), jnp.arange(PART_DEV), side="right"))(jax.random.split(streams_of[2], N_ROT)).reshape((N_ROT, PART_DEV)).astype(jnp.int32)
    ctf = jnp.clip(jax.random.uniform(streams_of[3], (MICS, CYCLES), jnp.float32, -1.0, 1.0) * levels(streams_of[3], (MICS, CYCLES), ((0, 8),), -0.4, 0.0), -1.0, 1.0)
    prior_class = place_ends(jax.random.randint(streams_of[4], (PARTICLES,), 0, CLASSES), jax.random.fold_in(streams_of[4], 1), 0, CLASSES - 1).astype(jnp.int32)
    return dict(particles=particles, references=references, micrograph=micrograph, ctf=ctf, prior_class=prior_class)


def reference(particles, references, micrograph, ctf, prior_class):
    particle_spectra = particles.astype(jnp.float32).reshape(PARTICLES, CYCLES, 2 * POLAR)
    rotation_energy = lax.optimization_barrier(jnp.mean(particle_spectra * particle_spectra, axis=2)).reshape(N_ROT, PART_DEV, CYCLES)
    indicator_matrix = (micrograph[:, :, None] == jnp.arange(MICS_DEV, dtype=jnp.int32)[None, None, :]).astype(jnp.float32)
    score_totals = jnp.einsum('ekn,ekx->enx', indicator_matrix, rotation_energy, precision=lax.Precision.HIGHEST)
    counts = lax.optimization_barrier(jnp.sum(indicator_matrix, axis=1))
    mean_power = score_totals / counts[:, :, None]
    scaling_coefficient = ctf.reshape(N_ROT, MICS_DEV, CYCLES) * lax.rsqrt(mean_power + 1e-06)
    particle_scores = jnp.einsum('usn,uno->uso', indicator_matrix, scaling_coefficient, precision=lax.Precision.HIGHEST)
    particle_scores = particle_scores.reshape(PARTICLES, CYCLES)
    whitened = (particle_spectra * particle_scores[:, :, None]).reshape(PARTICLES, F).astype(jnp.bfloat16)

    def class_best(class_templates):
        scored = jnp.dot(class_templates, whitened.T, preferred_element_type=jnp.float32)
        return lax.optimization_barrier(jnp.max(scored, axis=0))
    per_class = lax.map(class_best, references)
    class_scores = per_class.T
    best_score = lax.optimization_barrier(jnp.max(class_scores, axis=1))
    prior_score = jnp.take_along_axis(class_scores, prior_class[:, None].astype(jnp.int32), axis=1)[:, 0]
    return (class_scores, best_score, prior_score)
```

```python
import functools
import jax
import jax.numpy as jnp
from jax import lax
from jax.experimental import pallas as pl
from jax.experimental.pallas import tpu as pltpu
from jax.sharding import PartitionSpec as P

CYCLES = 64
LOW = -1e30
VMEM_BYTES = 62 * 1024 * 1024


def plan(n_rot, n_cls):
    ys = 2 if n_rot % 2 == 0 else 1
    cs = 2 if n_cls % 2 == 0 else 1
    units = max(1, 64 // n_rot)
    crossing = (3 * units) // 8 if n_cls == 2 * cs else 0
    return n_rot // ys, ys, n_cls // cs, cs, units, crossing


def kernel(n_rot, n_cls, part_ref, ref_ref, mic_ref, ctf_ref, prior_ref,
           cls_out, best_out, prior_out,
           g, refs_v, refs_p, acc, fac, fac_t, cs_tx, cs_rx, bp,
           own_sem, ref_sem, recv_sem, send_sem, fac_send, fac_recv,
           sc_send, sc_recv, bp_send, bp_recv):
    zs, ys, xs, cores, units, crossing = plan(n_rot, n_cls)
    through = units - crossing
    parts, feats = part_ref.shape
    classes, angles, _ = ref_ref.shape
    width = feats // (cores * units)
    step = feats // CYCLES
    rot = lax.axis_index("rot")
    cls = lax.axis_index("cls")
    z, y = lax.div(rot, ys), lax.rem(rot, ys)
    x, core = lax.div(cls, cores), lax.rem(cls, cores)

    own = pltpu.make_async_copy(part_ref, g.at[rot], own_sem)
    own.start()
    ref_copies = [
        pltpu.make_async_copy(ref_ref.at[c], refs_v.at[c], ref_sem.at[c]) for c in range(classes)
    ]
    for copy in ref_copies:
        copy.start()

    barrier = pltpu.get_barrier_semaphore()
    for d in range(1, n_rot):
        pl.semaphore_signal(barrier, inc=1, device_id=(lax.rem(rot + d, n_rot), cls),
                            device_id_type=pl.DeviceIdType.MESH)
    for d in range(1, n_cls):
        pl.semaphore_signal(barrier, inc=1, device_id=(rot, lax.rem(cls + d, n_cls)),
                            device_id_type=pl.DeviceIdType.MESH)
    pl.semaphore_wait(barrier, n_rot + n_cls - 2)

    def unit_of(j):
        return jnp.where(x == 0, j, units - 1 - j) if crossing else j

    def piece(shard, unit, half, dev, kind):
        col = pl.multiple_of((half * units + unit) * width, 128)
        ref = g.at[shard, :, pl.ds(col, width)]
        return pltpu.make_async_remote_copy(
            src_ref=ref, dst_ref=ref,
            send_sem=send_sem.at[kind, shard, unit],
            recv_sem=recv_sem.at[shard, half * units + unit],
            device_id=dev, device_id_type=pl.DeviceIdType.MESH)

    up, down = ((z + 1) * ys + y, cls), ((z - 1) * ys + y, cls)
    across = (z * ys + (ys - 1 - y), cls)
    other_x = (rot, (xs - 1 - x) * cores + core)
    mate = (rot, x * cores + (cores - 1 - core))
    UP, DOWN, ACROSS, OTHER, MATE = range(5)

    def send(shard, unit, dev, kind):
        piece(shard, unit, core, dev, kind).start()

    def sent(shard, unit, dev, kind):
        piece(shard, unit, core, dev, kind).wait_send()

    def to_chip(act, shard, j, j_is_far=False):
        if j < crossing:
            act(shard, unit_of(j), other_x, OTHER)
        if cores == 2:
            act(shard, unit_of(j), mate, MATE)

    def arrive(shard, unit, half):
        piece(shard, unit, half, mate, MATE).wait_recv()

    def when(cond, fn):
        pl.when(cond)(fn)

    def z_visit(d, j, sign, act, wait):
        shard = (z - sign * d) * ys + y
        exists = (z >= d) if sign > 0 else (z + d < zs)

        def visit():
            if wait:
                arrive(shard, unit_of(j), core)
            more = (z + 1 < zs) if sign > 0 else (z >= 1)
            if d < zs - 1:
                @pl.when(more)
                def _():
                    act(shard, unit_of(j), up if sign > 0 else down, UP if sign > 0 else DOWN)
            if ys == 2:
                act(shard, unit_of(j), across, ACROSS)
            to_chip(act, shard, j)
        when(exists, visit)

    def y_visit(d, j, sign, act, wait):
        shard = (z - sign * d) * ys + (ys - 1 - y)

        def visit():
            if wait:
                arrive(shard, unit_of(j), core)
            to_chip(act, shard, j)
        if d == 0:
            visit()
        else:
            when((z >= d) if sign > 0 else (z + d < zs), visit)

    def x_visit(d, j, sign, row, act, wait):
        shard = (z - sign * d) * ys + row
        unit = unit_of(units - 1 - j)

        def visit():
            if wait:
                arrive(shard, unit, core)
            if cores == 2:
                act(shard, unit, mate, MATE)
        if d == 0:
            visit()
        else:
            when((z >= d) if sign > 0 else (z + d < zs), visit)

    def first(j, act):
        @pl.when(z + 1 < zs)
        def _():
            act(rot, unit_of(j), up, UP)

        @pl.when(z >= 1)
        def _():
            act(rot, unit_of(j), down, DOWN)
        if ys == 2:
            act(rot, unit_of(j), across, ACROSS)

    def slot(r, j, act, wait):
        signs = (1, -1)
        if r == 0:
            first(j, act)
        if 1 <= r <= zs - 1:
            for sign in signs:
                z_visit(r, j, sign, act, wait)
        if 1 <= r <= zs and ys == 2:
            for sign in (signs if r > 1 else (1,)):
                y_visit(r - 1, j, sign, act, wait)
        if j < crossing:
            if 2 <= r <= zs:
                for sign in signs:
                    x_visit(r - 1, j, sign, y, act, wait)
            if 2 <= r <= zs + 1 and ys == 2:
                for sign in (signs if r > 2 else (1,)):
                    x_visit(r - 2, j, sign, ys - 1 - y, act, wait)

    own.wait()
    for j in range(through):
        slot(0, j, send, True)

    lane = lax.broadcasted_iota(jnp.int32, (parts, 128), 1)
    power = jnp.zeros((parts, 128), jnp.float32)
    for r in range(CYCLES):
        v = part_value(g, rot, r, step)
        power = jnp.where(lane == r, jnp.sum(v * v, axis=1, keepdims=True) / step, power)
    power = power[:, :CYCLES]
    eye = (lax.broadcasted_iota(jnp.int32, (parts, parts), 0)
           == lax.broadcasted_iota(jnp.int32, (parts, parts), 1))
    mic_row = jnp.broadcast_to(mic_ref[...].astype(jnp.float32), (parts, parts))
    mic_col = jnp.sum(jnp.where(eye, mic_row, 0.0), axis=1, keepdims=True)
    same = (mic_row == mic_col).astype(jnp.float32)
    mean = jnp.dot(same, power, precision=lax.Precision.HIGHEST,
                   preferred_element_type=jnp.float32)
    mean = mean / jnp.sum(same, axis=1, keepdims=True)
    ctf = ctf_ref[...]
    ctf_part = jnp.zeros((parts, CYCLES), jnp.float32)
    for m in range(ctf.shape[0]):
        ctf_part = jnp.where(mic_col == float(m), ctf[m:m + 1, :], ctf_part)
    factor = ctf_part * lax.rsqrt(mean + 1e-6)
    fac[rot] = jnp.concatenate([factor, jnp.zeros((parts, 128 - CYCLES), jnp.float32)], axis=1)

    for copy in ref_copies:
        copy.wait()

    def pad_block(i, carry):
        cols = pl.ds(pl.multiple_of(i * 1024, 1024), 1024)
        for c in range(classes):
            refs_p[c, 0:angles, cols] = refs_v[c, :, cols]
        return carry
    lax.fori_loop(0, feats // 1024, pad_block, 0)

    def fac_copy(d, shard):
        return pltpu.make_async_remote_copy(
            src_ref=fac.at[shard], dst_ref=fac.at[shard], send_sem=fac_send.at[d],
            recv_sem=fac_recv.at[shard], device_id=(lax.rem(rot + d, n_rot), cls),
            device_id_type=pl.DeviceIdType.MESH)
    for d in range(1, n_rot):
        fac_copy(d, rot).start()

    for r in range(1, zs + 2):
        for j in range(through):
            slot(r, j, send, True)

    if cores == 2:
        for d in range(1, n_rot):
            shard = lax.rem(rot + d, n_rot)
            for u in range(units):
                arrive(shard, u, 1 - core)
    for d in range(1, n_rot):
        fac_copy(d, lax.rem(rot + n_rot - d, n_rot)).wait_recv()

    total = n_rot * parts
    fac_t[...] = fac[...].reshape(total, 128).T
    rows = refs_p.shape[0] * refs_p.shape[1]
    acc[...] = jnp.zeros_like(acc)

    def cycle_block(i, carry):
        part_sum = None
        for k in range(4):
            r = i * 4 + k
            cols = pl.ds(pl.multiple_of(r * step, 128), step)
            dot = lax.dot_general(
                refs_p[:, :, cols].reshape(rows, step), g[:, :, cols].reshape(total, step),
                (((1,), (1,)), ((), ())), preferred_element_type=jnp.float32)
            dot = dot * fac_t[pl.ds(r, 1), :]
            part_sum = dot if part_sum is None else part_sum + dot
        acc[...] += part_sum
        return carry
    lax.fori_loop(0, CYCLES // 4, cycle_block, 0)

    score = acc[...].reshape(classes, refs_p.shape[1], total)
    angle = lax.broadcasted_iota(jnp.int32, score.shape, 1)
    local = jnp.max(jnp.where(angle < angles, score, LOW), axis=1)
    local = jnp.concatenate([local, jnp.full((128 - classes, total), LOW, jnp.float32)], axis=0)
    cs_tx[...] = local.T.reshape(n_rot, parts, 128)

    def score_copy(d, block, slot_):
        return pltpu.make_async_remote_copy(
            src_ref=cs_tx.at[block], dst_ref=cs_rx.at[slot_], send_sem=sc_send.at[d],
            recv_sem=sc_recv.at[slot_], device_id=(lax.rem(rot + d, n_rot), cls),
            device_id_type=pl.DeviceIdType.MESH)
    for d in range(1, n_rot):
        score_copy(d, lax.rem(rot + d, n_rot), rot).start()
    best = cs_tx[rot]
    for d in range(1, n_rot):
        src = lax.rem(rot + n_rot - d, n_rot)
        score_copy(d, rot, src).wait_recv()
        best = jnp.maximum(best, cs_rx[src])
    cls_out[...] = best[:, :classes]

    prior_row = jnp.broadcast_to(prior_ref[...], (parts, parts))
    prior_col = jnp.sum(jnp.where(eye, prior_row, 0), axis=1, keepdims=True)
    chosen = (prior_col == lane + cls * classes) & (lane < classes)
    top = jnp.max(best, axis=1, keepdims=True)
    earlier = jnp.max(jnp.where(chosen, best, LOW), axis=1, keepdims=True)
    bp[cls] = jnp.where(lane == 0, top, earlier)

    def bp_copy(d, slot_):
        return pltpu.make_async_remote_copy(
            src_ref=bp.at[slot_], dst_ref=bp.at[slot_], send_sem=bp_send.at[d],
            recv_sem=bp_recv.at[slot_], device_id=(rot, lax.rem(cls + d, n_cls)),
            device_id_type=pl.DeviceIdType.MESH)
    for d in range(1, n_cls):
        bp_copy(d, cls).start()
    both = bp[cls]
    for d in range(1, n_cls):
        src = lax.rem(cls + n_cls - d, n_cls)
        bp_copy(d, src).wait_recv()
        both = jnp.maximum(both, bp[src])
    best_out[...] = jnp.max(jnp.where(eye, both[:, 0:1], LOW), axis=0, keepdims=True)
    prior_out[...] = jnp.max(jnp.where(eye, both[:, 1:2], LOW), axis=0, keepdims=True)

    for r in range(zs + 2):
        for j in range(through):
            slot(r, j, sent, False)
    for d in range(1, n_rot):
        fac_copy(d, rot).wait_send()
        score_copy(d, rot, rot).wait_send()
    for d in range(1, n_cls):
        bp_copy(d, cls).wait_send()


def part_value(g, rot, r, step):
    return g[rot, :, r * step:(r + 1) * step].astype(jnp.float32)


def body(n_rot, n_cls, particles, references, micrograph, ctf, prior_class):
    parts, feats = particles.shape
    classes, angles, _ = references.shape
    padded = -(-angles // 16) * 16
    units = plan(n_rot, n_cls)[4]
    vmem = pl.BlockSpec(memory_space=pltpu.VMEM)
    hbm = pl.BlockSpec(memory_space=pl.ANY)
    dma = pltpu.SemaphoreType.DMA
    total = n_rot * parts
    out = pl.pallas_call(
        functools.partial(kernel, n_rot, n_cls),
        out_shape=(jax.ShapeDtypeStruct((parts, classes), jnp.float32),
                   jax.ShapeDtypeStruct((1, parts), jnp.float32),
                   jax.ShapeDtypeStruct((1, parts), jnp.float32)),
        in_specs=[hbm, hbm, vmem, vmem, vmem],
        out_specs=(vmem, vmem, vmem),
        scratch_shapes=[
            pltpu.VMEM((n_rot, parts, feats), jnp.bfloat16),
            pltpu.VMEM((classes, angles, feats), jnp.bfloat16),
            pltpu.VMEM((classes, padded, feats), jnp.bfloat16),
            pltpu.VMEM((classes * padded, total), jnp.float32),
            pltpu.VMEM((n_rot, parts, 128), jnp.float32),
            pltpu.VMEM((128, total), jnp.float32),
            pltpu.VMEM((n_rot, parts, 128), jnp.float32),
            pltpu.VMEM((n_rot, parts, 128), jnp.float32),
            pltpu.VMEM((n_cls, parts, 128), jnp.float32),
            dma, dma((classes,)), dma((n_rot, 2 * units)), dma((5, n_rot, units)),
            dma((n_rot,)), dma((n_rot,)), dma((n_rot,)), dma((n_rot,)),
            dma((n_cls,)), dma((n_cls,)),
        ],
        compiler_params=pltpu.CompilerParams(
            collective_id=0, has_side_effects=True, vmem_limit_bytes=VMEM_BYTES),
    )(particles, references, micrograph, ctf, prior_class.reshape(1, parts))
    return out[0], out[1].reshape(parts), out[2].reshape(parts)


def solution(mesh):
    in_specs = (P("rot", None), P("cls", "rot", None), P("rot", None), P("rot", None), P("rot"))
    out_specs = (P("rot", "cls"), P("rot"), P("rot"))
    fn = functools.partial(body, mesh.shape["rot"], mesh.shape["cls"])
    return jax.shard_map(fn, mesh=mesh, in_specs=in_specs, out_specs=out_specs, check_vma=False)
```

```python
import functools
import jax
import jax.numpy as jnp
from jax import lax
from jax.experimental import pallas as pl
from jax.experimental.pallas import tpu as pltpu
from jax.sharding import PartitionSpec as P

CYCLES = 64
LOW = -1e30
EDGE, MIDS = 6, 1
VMEM_BYTES = 62 * 1024 * 1024


def plan(n_rot, n_cls):
    ys = 2 if n_rot % 2 == 0 else 1
    cs = 2 if n_cls % 2 == 0 else 1
    half = CYCLES // cs
    if n_cls == 2 * cs and n_rot <= 16:
        edge = (EDGE * half) // 32
        mid = half - 4 * edge
        mids = [mid // MIDS] * MIDS
        widths, crossing = [edge, edge] + mids + [edge, edge], 2
    else:
        widths, crossing = [half], 0
    assert sum(widths) == half
    return n_rot // ys, ys, n_cls // cs, cs, widths, crossing


def kernel(n_rot, n_cls, part_ref, ref_ref, mic_ref, ctf_ref, prior_ref,
           res_out,
           g, refs_v, refs_p, acc, fac, fac_t, cs_tx, cs_rx, bp,
           own_sem, ref_sem, recv_sem, send_sem, fac_send, fac_recv,
           sc_send, sc_recv, bp_send, bp_recv):
    zs, ys, xs, cores, widths, crossing = plan(n_rot, n_cls)
    units = len(widths)
    through = units - crossing
    fac_at = min(2, through - 1)
    starts = [sum(widths[:u]) for u in range(units)]
    half_cycles = CYCLES // cores
    parts, feats = part_ref.shape
    classes, angles, _ = ref_ref.shape
    step = feats // CYCLES
    rot = lax.axis_index("rot")
    cls = lax.axis_index("cls")
    z, y = lax.div(rot, ys), lax.rem(rot, ys)
    x, core = lax.div(cls, cores), lax.rem(cls, cores)

    own = pltpu.make_async_copy(part_ref, g.at[rot], own_sem)
    own.start()
    ref_copies = [
        pltpu.make_async_copy(ref_ref.at[c], refs_v.at[c], ref_sem.at[c]) for c in range(classes)
    ]
    for copy in ref_copies:
        copy.start()

    up, down = ((z + 1) * ys + y, cls), ((z - 1) * ys + y, cls)
    across = (z * ys + (ys - 1 - y), cls)
    other_x = (rot, (xs - 1 - x) * cores + core)
    mate = (rot, x * cores + (cores - 1 - core))
    has_up, has_down = z + 1 < zs, z >= 1
    UP, DOWN, ACROSS, OTHER, MATE = range(5)

    barrier = pltpu.get_barrier_semaphore()

    def greet(dev):
        pl.semaphore_signal(barrier, inc=1, device_id=dev,
                            device_id_type=pl.DeviceIdType.MESH)
    near = ([across] if ys == 2 else []) + ([other_x] if crossing else [])
    near += [mate] if cores == 2 else []
    pl.when(has_up)(lambda: greet(up))
    pl.when(has_down)(lambda: greet(down))
    for dev in near:
        greet(dev)
    pl.semaphore_wait(
        barrier, len(near) + jnp.where(has_up, 1, 0) + jnp.where(has_down, 1, 0))

    def unit_of(j):
        return jnp.where(x == 0, j, units - 1 - j) if crossing else j

    def cycle_of(j, half):
        first_cycle = jnp.where(x == 0, starts[j], starts[units - 1 - j]) if crossing else starts[j]
        return half * half_cycles + first_cycle

    def piece(shard, j, half, dev, kind):
        col = pl.multiple_of(cycle_of(j, half) * step, step)
        ref = g.at[shard, :, pl.ds(col, widths[j] * step)]
        unit = unit_of(j)
        return pltpu.make_async_remote_copy(
            src_ref=ref, dst_ref=ref,
            send_sem=send_sem.at[kind, shard, unit],
            recv_sem=recv_sem.at[shard, half * units + unit],
            device_id=dev, device_id_type=pl.DeviceIdType.MESH)

    def fac_copy(shard, dev, kind):
        return pltpu.make_async_remote_copy(
            src_ref=fac.at[shard], dst_ref=fac.at[shard], send_sem=fac_send.at[kind, shard],
            recv_sem=fac_recv.at[shard], device_id=dev, device_id_type=pl.DeviceIdType.MESH)

    def send(shard, j, dev, kind):
        piece(shard, j, core, dev, kind).start()

    def sent(shard, j, dev, kind):
        piece(shard, j, core, dev, kind).wait_send()

    def send_fac(shard, dev, kind):
        fac_copy(shard, dev, kind).start()

    def sent_fac(shard, dev, kind):
        fac_copy(shard, dev, kind).wait_send()

    def to_chip(act, shard, j):
        if j < crossing:
            act(shard, j, other_x, OTHER)
        if cores == 2:
            act(shard, j, mate, MATE)

    def arrive(shard, j, half):
        piece(shard, j, half, mate, MATE).wait_recv()

    def z_visit(d, j, sign, act, wait):
        shard = (z - sign * d) * ys + y
        exists = (z >= d) if sign > 0 else (z + d < zs)

        def visit():
            if wait:
                arrive(shard, j, core)
            more, dev, kind = (has_up, up, UP) if sign > 0 else (has_down, down, DOWN)
            if d < zs - 1:
                pl.when(more)(lambda: act(shard, j, dev, kind))
            if ys == 2:
                act(shard, j, across, ACROSS)
            to_chip(act, shard, j)
            if j == fac_at:
                if wait:
                    fac_copy(shard, mate, 0).wait_recv()
                fac_act = send_fac if wait else sent_fac
                if d < zs - 1:
                    pl.when(more)(lambda: fac_act(shard, dev, kind))
                if ys == 2:
                    fac_act(shard, across, ACROSS)
        pl.when(exists)(visit)

    def y_visit(d, j, sign, act, wait):
        shard = (z - sign * d) * ys + (ys - 1 - y)

        def visit():
            if wait:
                arrive(shard, j, core)
            to_chip(act, shard, j)
            if j == fac_at and wait:
                fac_copy(shard, mate, 0).wait_recv()
        if d == 0:
            visit()
        else:
            pl.when((z >= d) if sign > 0 else (z + d < zs))(visit)

    def x_visit(d, j, sign, row, act, wait):
        shard = (z - sign * d) * ys + row
        far = units - 1 - j

        def visit():
            if wait:
                arrive(shard, far, core)
            if cores == 2:
                act(shard, far, mate, MATE)
        if d == 0:
            visit()
        else:
            pl.when((z >= d) if sign > 0 else (z + d < zs))(visit)

    def first(act_on):
        pl.when(has_up)(lambda: act_on(up, UP))
        pl.when(has_down)(lambda: act_on(down, DOWN))
        if ys == 2:
            act_on(across, ACROSS)

    def slot(r, j, act, wait):
        signs = (1, -1)
        if r == 0:
            first(lambda dev, kind: act(rot, j, dev, kind))
        if 1 <= r <= zs - 1:
            for sign in signs:
                z_visit(r, j, sign, act, wait)
        if 1 <= r <= zs and ys == 2:
            for sign in (signs if r > 1 else (1,)):
                y_visit(r - 1, j, sign, act, wait)
        if j < crossing:
            if 2 <= r <= zs:
                for sign in signs:
                    x_visit(r - 1, j, sign, y, act, wait)
            if 2 <= r <= zs + 1 and ys == 2:
                for sign in (signs if r > 2 else (1,)):
                    x_visit(r - 2, j, sign, ys - 1 - y, act, wait)

    own.wait()
    for j in range(min(2, through)):
        slot(0, j, send, True)

    lane = lax.broadcasted_iota(jnp.int32, (parts, 128), 1)
    power = jnp.zeros((parts, 128), jnp.float32)
    for r in range(CYCLES):
        v = part_value(g, rot, r, step)
        power = jnp.where(lane == r, jnp.sum(v * v, axis=1, keepdims=True) / step, power)
    power = power[:, :CYCLES]
    eye = (lax.broadcasted_iota(jnp.int32, (parts, parts), 0)
           == lax.broadcasted_iota(jnp.int32, (parts, parts), 1))
    mic_row = jnp.broadcast_to(mic_ref[...].astype(jnp.float32), (parts, parts))
    mic_col = jnp.sum(jnp.where(eye, mic_row, 0.0), axis=1, keepdims=True)
    same = (mic_row == mic_col).astype(jnp.float32)
    mean = jnp.dot(same, power, precision=lax.Precision.HIGHEST,
                   preferred_element_type=jnp.float32)
    mean = mean / jnp.sum(same, axis=1, keepdims=True)
    ctf = ctf_ref[...]
    ctf_part = jnp.zeros((parts, CYCLES), jnp.float32)
    for m in range(ctf.shape[0]):
        ctf_part = jnp.where(mic_col == float(m), ctf[m:m + 1, :], ctf_part)
    factor = ctf_part * lax.rsqrt(mean + 1e-6)
    fac[rot] = jnp.concatenate([factor, jnp.zeros((parts, 128 - CYCLES), jnp.float32)], axis=1)
    acc[...] = jnp.zeros_like(acc)
    for j in range(min(2, through), fac_at + 1):
        slot(0, j, send, True)
    first(lambda dev, kind: send_fac(rot, dev, kind))
    for j in range(fac_at + 1, through):
        slot(0, j, send, True)

    for copy in ref_copies:
        copy.wait()

    def pad_block(i, carry):
        cols = pl.ds(pl.multiple_of(i * 1024, 1024), 1024)
        for c in range(classes):
            refs_p[c, 0:angles, cols] = refs_v[c, :, cols]
        return carry
    lax.fori_loop(0, feats // 1024, pad_block, 0)

    for r in range(1, zs):
        for j in range(through):
            slot(r, j, send, True)

    total = n_rot * parts
    rows = refs_p.shape[0] * refs_p.shape[1]

    def cycles_dot(first_cycle, count):
        part_sum = None
        for k in range(count):
            r = first_cycle + k
            cols = pl.ds(pl.multiple_of(r * step, step), step)
            dot = lax.dot_general(
                refs_p[:, :, cols].reshape(rows, step), g[:, :, cols].reshape(total, step),
                (((1,), (1,)), ((), ())), preferred_element_type=jnp.float32)
            dot = dot * fac_t[pl.ds(r, 1), :]
            part_sum = dot if part_sum is None else part_sum + dot
        acc[...] += part_sum

    def compute(j, half):
        if widths[j] <= 8:
            cycles_dot(cycle_of(j, half), widths[j])
        else:
            lax.fori_loop(
                0, widths[j], lambda i, c: (cycles_dot(cycle_of(j, half) + i, 1), c)[1], 0)

    def mate_units(j):
        for d in range(1, n_rot):
            arrive(lax.rem(rot + d, n_rot), j, 1 - core)
        compute(j, 1 - core)

    for j in range(fac_at + 1):
        slot(zs, j, send, True)
    fac_t[...] = fac[...].reshape(total, 128).T
    for j in range(fac_at):
        compute(j, core)
    for j in range(fac_at + 1, through):
        slot(zs, j, send, True)
    for j in range(crossing):
        slot(zs + 1, j, send, True)
    for j in range(fac_at, through):
        compute(j, core)
    for j in range(crossing):
        compute(units - 1 - j, core)
    if cores == 2:
        for j in range(units):
            mate_units(j)

    score = acc[...].reshape(classes, refs_p.shape[1], total)
    angle = lax.broadcasted_iota(jnp.int32, score.shape, 1)
    local = jnp.max(jnp.where(angle < angles, score, LOW), axis=1)
    local = jnp.concatenate([local, jnp.full((128 - classes, total), LOW, jnp.float32)], axis=0)
    cs_tx[...] = local.T.reshape(n_rot, parts, 128)

    def score_copy(d, block, slot_):
        return pltpu.make_async_remote_copy(
            src_ref=cs_tx.at[block], dst_ref=cs_rx.at[slot_], send_sem=sc_send.at[d],
            recv_sem=sc_recv.at[slot_], device_id=(lax.rem(rot + d, n_rot), cls),
            device_id_type=pl.DeviceIdType.MESH)
    for d in range(1, n_rot):
        score_copy(d, lax.rem(rot + d, n_rot), rot).start()
    for r in range(zs + 2):
        for j in range(through):
            slot(r, j, sent, False)
    first(lambda dev, kind: sent_fac(rot, dev, kind))
    best = cs_tx[rot]
    for d in range(1, n_rot):
        src = lax.rem(rot + n_rot - d, n_rot)
        score_copy(d, rot, src).wait_recv()
        best = jnp.maximum(best, cs_rx[src])

    prior_row = jnp.broadcast_to(prior_ref[...], (parts, parts))
    prior_col = jnp.sum(jnp.where(eye, prior_row, 0), axis=1, keepdims=True)
    chosen = (prior_col == lane + cls * classes) & (lane < classes)
    top = jnp.max(best, axis=1, keepdims=True)
    earlier = jnp.max(jnp.where(chosen, best, LOW), axis=1, keepdims=True)
    bp[cls] = jnp.where(lane == 0, top, earlier)

    def bp_copy(d, slot_):
        return pltpu.make_async_remote_copy(
            src_ref=bp.at[slot_], dst_ref=bp.at[slot_], send_sem=bp_send.at[d],
            recv_sem=bp_recv.at[slot_], device_id=(rot, lax.rem(cls + d, n_cls)),
            device_id_type=pl.DeviceIdType.MESH)
    for d in range(1, n_cls):
        bp_copy(d, cls).start()
    both = bp[cls]
    for d in range(1, n_cls):
        src = lax.rem(cls + n_cls - d, n_cls)
        bp_copy(d, src).wait_recv()
        both = jnp.maximum(both, bp[src])
    res_out[...] = jnp.where(lane == 126, both[:, 0:1], jnp.where(lane == 127, both[:, 1:2], best))
    for d in range(1, n_rot):
        score_copy(d, rot, rot).wait_send()
    for d in range(1, n_cls):
        bp_copy(d, cls).wait_send()


def finish(res_ref, cls_out, best_out, prior_out):
    res = res_ref[...]
    parts, classes = cls_out.shape
    cls_out[...] = res[:, :classes]
    eye = (lax.broadcasted_iota(jnp.int32, (parts, parts), 0)
           == lax.broadcasted_iota(jnp.int32, (parts, parts), 1))
    best_out[...] = jnp.max(jnp.where(eye, res[:, 126:127], LOW), axis=0, keepdims=True)
    prior_out[...] = jnp.max(jnp.where(eye, res[:, 127:128], LOW), axis=0, keepdims=True)


def part_value(g, rot, r, step):
    return g[rot, :, r * step:(r + 1) * step].astype(jnp.float32)


def body(n_rot, n_cls, particles, references, micrograph, ctf, prior_class):
    parts, feats = particles.shape
    classes, angles, _ = references.shape
    padded = -(-angles // 16) * 16
    units = len(plan(n_rot, n_cls)[4])
    vmem = pl.BlockSpec(memory_space=pltpu.VMEM)
    hbm = pl.BlockSpec(memory_space=pl.ANY)
    dma = pltpu.SemaphoreType.DMA
    total = n_rot * parts
    res = pl.pallas_call(
        functools.partial(kernel, n_rot, n_cls),
        out_shape=jax.ShapeDtypeStruct((parts, 128), jnp.float32),
        in_specs=[hbm, hbm, vmem, vmem, vmem],
        out_specs=vmem,
        scratch_shapes=[
            pltpu.VMEM((n_rot, parts, feats), jnp.bfloat16),
            pltpu.VMEM((classes, angles, feats), jnp.bfloat16),
            pltpu.VMEM((classes, padded, feats), jnp.bfloat16),
            pltpu.VMEM((classes * padded, total), jnp.float32),
            pltpu.VMEM((n_rot, parts, 128), jnp.float32),
            pltpu.VMEM((128, total), jnp.float32),
            pltpu.VMEM((n_rot, parts, 128), jnp.float32),
            pltpu.VMEM((n_rot, parts, 128), jnp.float32),
            pltpu.VMEM((n_cls, parts, 128), jnp.float32),
            dma, dma((classes,)), dma((n_rot, 2 * units)), dma((5, n_rot, units)),
            dma((3, n_rot)), dma((n_rot,)), dma((n_rot,)), dma((n_rot,)),
            dma((n_cls,)), dma((n_cls,)),
        ],
        compiler_params=pltpu.CompilerParams(
            collective_id=0, has_side_effects=True, vmem_limit_bytes=VMEM_BYTES),
    )(particles, references, micrograph, ctf, prior_class.reshape(1, parts))
    out = pl.pallas_call(
        finish,
        out_shape=(jax.ShapeDtypeStruct((parts, classes), jnp.float32),
                   jax.ShapeDtypeStruct((1, parts), jnp.float32),
                   jax.ShapeDtypeStruct((1, parts), jnp.float32)),
        in_specs=[vmem], out_specs=(vmem, vmem, vmem),
    )(res)
    return out[0], out[1].reshape(parts), out[2].reshape(parts)


def solution(mesh):
    in_specs = (P("rot", None), P("cls", "rot", None), P("rot", None), P("rot", None), P("rot"))
    out_specs = (P("rot", "cls"), P("rot"), P("rot"))
    fn = functools.partial(body, mesh.shape["rot"], mesh.shape["cls"])
    return jax.shard_map(fn, mesh=mesh, in_specs=in_specs, out_specs=out_specs, check_vma=False)
```

```python
import functools
import jax
import jax.numpy as jnp
from jax import lax
from jax.experimental import pallas as pl
from jax.experimental.pallas import tpu as pltpu
from jax.sharding import PartitionSpec as P

CYCLES = 64
LOW = -1e30
EDGE, MIDS = 6, 1
XLAG, YLAG = 2, 3
VMEM_BYTES = 62 * 1024 * 1024


def plan(n_rot, n_cls):
    ys = 2 if n_rot % 2 == 0 else 1
    cs = 2 if n_cls % 2 == 0 else 1
    half = CYCLES // cs
    if n_cls == 2 * cs and n_rot <= 16:
        edge = (EDGE * half) // 32
        mid = half - 4 * edge
        mids = [mid // MIDS] * MIDS
        widths, crossing = [edge, edge] + mids + [edge, edge], 2
    else:
        widths, crossing = [half], 0
    assert sum(widths) == half
    return n_rot // ys, ys, n_cls // cs, cs, widths, crossing


def kernel(n_rot, n_cls, part_ref, ref_ref, mic_ref, ctf_ref, prior_ref,
           res_out,
           g, refs_v, refs_p, acc, fac, fac_t, cs_tx, cs_rx, bp,
           own_sem, ref_sem, recv_sem, send_sem, fac_send, fac_recv,
           sc_send, sc_recv, bp_send, bp_recv):
    zs, ys, xs, cores, widths, crossing = plan(n_rot, n_cls)
    units = len(widths)
    through = units - crossing
    fac_at = min(1, through - 1)
    starts = [sum(widths[:u]) for u in range(units)]
    half_cycles = CYCLES // cores
    parts, feats = part_ref.shape
    classes, angles, _ = ref_ref.shape
    step = feats // CYCLES
    rot = lax.axis_index("rot")
    cls = lax.axis_index("cls")
    z, y = lax.div(rot, ys), lax.rem(rot, ys)
    x, core = lax.div(cls, cores), lax.rem(cls, cores)

    own = pltpu.make_async_copy(part_ref, g.at[rot], own_sem)
    own.start()
    ref_copies = [
        pltpu.make_async_copy(ref_ref.at[c], refs_v.at[c], ref_sem.at[c]) for c in range(classes)
    ]
    for copy in ref_copies:
        copy.start()

    up, down = ((z + 1) * ys + y, cls), ((z - 1) * ys + y, cls)
    across = (z * ys + (ys - 1 - y), cls)
    other_x = (rot, (xs - 1 - x) * cores + core)
    mate = (rot, x * cores + (cores - 1 - core))
    has_up, has_down = z + 1 < zs, z >= 1
    at_end = (z == 0) | (z == zs - 1)
    UP, DOWN, ACROSS, OTHER, MATE = range(5)

    barrier = pltpu.get_barrier_semaphore()

    def greet(dev):
        pl.semaphore_signal(barrier, inc=1, device_id=dev,
                            device_id_type=pl.DeviceIdType.MESH)
    near = ([across] if ys == 2 else []) + ([other_x] if crossing else [])
    near += [mate] if cores == 2 else []
    pl.when(has_up)(lambda: greet(up))
    pl.when(has_down)(lambda: greet(down))
    for dev in near:
        greet(dev)
    pl.semaphore_wait(
        barrier, len(near) + jnp.where(has_up, 1, 0) + jnp.where(has_down, 1, 0))

    def unit_of(j):
        return jnp.where(x == 0, j, units - 1 - j) if crossing else j

    def cycle_of(j, half):
        first_cycle = jnp.where(x == 0, starts[j], starts[units - 1 - j]) if crossing else starts[j]
        return half * half_cycles + first_cycle

    def piece(shard, j, half, dev, kind):
        col = pl.multiple_of(cycle_of(j, half) * step, step)
        ref = g.at[shard, :, pl.ds(col, widths[j] * step)]
        unit = unit_of(j)
        return pltpu.make_async_remote_copy(
            src_ref=ref, dst_ref=ref,
            send_sem=send_sem.at[kind, shard, unit],
            recv_sem=recv_sem.at[shard, half * units + unit],
            device_id=dev, device_id_type=pl.DeviceIdType.MESH)

    def fac_copy(shard, dev, kind):
        return pltpu.make_async_remote_copy(
            src_ref=fac.at[shard], dst_ref=fac.at[shard], send_sem=fac_send.at[kind, shard],
            recv_sem=fac_recv.at[shard], device_id=dev, device_id_type=pl.DeviceIdType.MESH)

    def send(shard, j, dev, kind):
        piece(shard, j, core, dev, kind).start()

    def sent(shard, j, dev, kind):
        piece(shard, j, core, dev, kind).wait_send()

    def send_fac(shard, dev, kind):
        fac_copy(shard, dev, kind).start()

    def sent_fac(shard, dev, kind):
        fac_copy(shard, dev, kind).wait_send()

    def to_chip(act, shard, j):
        if j < crossing:
            act(shard, j, other_x, OTHER)
        if cores == 2:
            act(shard, j, mate, MATE)

    def arrive(shard, j, half):
        piece(shard, j, half, mate, MATE).wait_recv()

    def z_visit(d, j, sign, act, wait):
        shard = (z - sign * d) * ys + y
        exists = (z >= d) if sign > 0 else (z + d < zs)

        def visit():
            if wait:
                arrive(shard, j, core)
            more, dev, kind = (has_up, up, UP) if sign > 0 else (has_down, down, DOWN)
            if d < zs - 1:
                pl.when(more)(lambda: act(shard, j, dev, kind))
            if ys == 2:
                act(shard, j, across, ACROSS)
            to_chip(act, shard, j)
            if j == fac_at:
                if wait:
                    fac_copy(shard, mate, 0).wait_recv()
                fac_act = send_fac if wait else sent_fac
                if d < zs - 1:
                    pl.when(more)(lambda: fac_act(shard, dev, kind))
                if ys == 2:
                    fac_act(shard, across, ACROSS)
        pl.when(exists)(visit)

    def y_visit(d, j, sign, act, wait, where):
        shard = (z - sign * d) * ys + (ys - 1 - y)

        def visit():
            if wait:
                arrive(shard, j, core)
            to_chip(act, shard, j)
            if j == fac_at and wait:
                fac_copy(shard, mate, 0).wait_recv()
        if d == 0:
            visit()
        else:
            pl.when(((z >= d) if sign > 0 else (z + d < zs)) & where)(visit)

    def x_visit(d, j, sign, row, act, wait):
        shard = (z - sign * d) * ys + row
        far = units - 1 - j

        def visit():
            if wait:
                arrive(shard, far, core)
            if cores == 2:
                act(shard, far, mate, MATE)
        if d == 0:
            visit()
        else:
            pl.when((z >= d) if sign > 0 else (z + d < zs))(visit)

    def first(act_on):
        pl.when(has_up)(lambda: act_on(up, UP))
        pl.when(has_down)(lambda: act_on(down, DOWN))
        if ys == 2:
            act_on(across, ACROSS)

    def slot(r, j, act, wait):
        signs = (1, -1)
        if r == 0:
            first(lambda dev, kind: act(rot, j, dev, kind))
        if 1 <= r <= zs - 1:
            for sign in signs:
                z_visit(r, j, sign, act, wait)
        if ys == 2:
            for d in range(zs):
                for sign in (signs if d else (1,)):
                    if r == d + 1:
                        y_visit(d, j, sign, act, wait, at_end if d else None)
                    if r == d + 2 and 1 <= d <= zs - 2:
                        y_visit(d, j, sign, act, wait, jnp.logical_not(at_end))
        if j < crossing:
            for d in range(zs):
                for sign in (signs if d else (1,)):
                    if d and r == d + XLAG:
                        x_visit(d, j, sign, y, act, wait)
                    if ys == 2 and r == min(d + YLAG, zs + 1):
                        x_visit(d, j, sign, ys - 1 - y, act, wait)

    own.wait()
    for j in range(min(2, through)):
        slot(0, j, send, True)

    lane = lax.broadcasted_iota(jnp.int32, (parts, 128), 1)
    power = jnp.zeros((parts, 128), jnp.float32)
    for r in range(CYCLES):
        v = part_value(g, rot, r, step)
        power = jnp.where(lane == r, jnp.sum(v * v, axis=1, keepdims=True) / step, power)
    power = power[:, :CYCLES]
    eye = (lax.broadcasted_iota(jnp.int32, (parts, parts), 0)
           == lax.broadcasted_iota(jnp.int32, (parts, parts), 1))
    mic_row = jnp.broadcast_to(mic_ref[...].astype(jnp.float32), (parts, parts))
    mic_col = jnp.sum(jnp.where(eye, mic_row, 0.0), axis=1, keepdims=True)
    same = (mic_row == mic_col).astype(jnp.float32)
    mean = jnp.dot(same, power, precision=lax.Precision.HIGHEST,
                   preferred_element_type=jnp.float32)
    mean = mean / jnp.sum(same, axis=1, keepdims=True)
    ctf = ctf_ref[...]
    ctf_part = jnp.zeros((parts, CYCLES), jnp.float32)
    for m in range(ctf.shape[0]):
        ctf_part = jnp.where(mic_col == float(m), ctf[m:m + 1, :], ctf_part)
    factor = ctf_part * lax.rsqrt(mean + 1e-6)
    fac[rot] = jnp.concatenate([factor, jnp.zeros((parts, 128 - CYCLES), jnp.float32)], axis=1)
    acc[...] = jnp.zeros_like(acc)
    for j in range(min(2, through), fac_at + 1):
        slot(0, j, send, True)
    first(lambda dev, kind: send_fac(rot, dev, kind))
    for j in range(fac_at + 1, through):
        slot(0, j, send, True)

    for copy in ref_copies:
        copy.wait()

    def pad_block(i, carry):
        cols = pl.ds(pl.multiple_of(i * 1024, 1024), 1024)
        for c in range(classes):
            refs_p[c, 0:angles, cols] = refs_v[c, :, cols]
        return carry
    lax.fori_loop(0, feats // 1024, pad_block, 0)

    for r in range(1, zs):
        for j in range(through):
            slot(r, j, send, True)

    total = n_rot * parts
    rows = refs_p.shape[0] * refs_p.shape[1]

    def cycles_dot(first_cycle, count):
        part_sum = None
        for k in range(count):
            r = first_cycle + k
            cols = pl.ds(pl.multiple_of(r * step, step), step)
            dot = lax.dot_general(
                refs_p[:, :, cols].reshape(rows, step), g[:, :, cols].reshape(total, step),
                (((1,), (1,)), ((), ())), preferred_element_type=jnp.float32)
            dot = dot * fac_t[pl.ds(r, 1), :]
            part_sum = dot if part_sum is None else part_sum + dot
        acc[...] += part_sum

    def compute(j, half):
        if widths[j] <= 8:
            cycles_dot(cycle_of(j, half), widths[j])
        else:
            lax.fori_loop(
                0, widths[j], lambda i, c: (cycles_dot(cycle_of(j, half) + i, 1), c)[1], 0)

    def mate_units(j):
        for d in range(1, n_rot):
            arrive(lax.rem(rot + d, n_rot), j, 1 - core)
        compute(j, 1 - core)

    for j in range(fac_at + 1):
        slot(zs, j, send, True)
    fac_t[...] = fac[...].reshape(total, 128).T
    early = fac_at + 1 if through > fac_at + 1 else 0
    for j in range(early):
        compute(j, core)
    if cores == 2 and early:
        mate_units(0)
    for j in range(fac_at + 1, through):
        slot(zs, j, send, True)
    for j in range(crossing):
        slot(zs + 1, j, send, True)
    if cores == 2:
        for j in range(min(early, 1), early):
            mate_units(j)
    for j in list(range(early, through)) + [units - 1 - j for j in range(crossing)]:
        compute(j, core)
    if cores == 2:
        for j in range(early, units):
            mate_units(j)

    score = acc[...].reshape(classes, refs_p.shape[1], total)
    angle = lax.broadcasted_iota(jnp.int32, score.shape, 1)
    local = jnp.max(jnp.where(angle < angles, score, LOW), axis=1)
    local = jnp.concatenate([local, jnp.full((128 - classes, total), LOW, jnp.float32)], axis=0)
    cs_tx[...] = local.T.reshape(n_rot, parts, 128)

    def score_copy(d, block, slot_):
        return pltpu.make_async_remote_copy(
            src_ref=cs_tx.at[block], dst_ref=cs_rx.at[slot_], send_sem=sc_send.at[d],
            recv_sem=sc_recv.at[slot_], device_id=(lax.rem(rot + d, n_rot), cls),
            device_id_type=pl.DeviceIdType.MESH)
    for d in range(1, n_rot):
        score_copy(d, lax.rem(rot + d, n_rot), rot).start()
    for r in range(zs + 2):
        for j in range(through):
            slot(r, j, sent, False)
    first(lambda dev, kind: sent_fac(rot, dev, kind))
    best = cs_tx[rot]
    for d in range(1, n_rot):
        src = lax.rem(rot + n_rot - d, n_rot)
        score_copy(d, rot, src).wait_recv()
        best = jnp.maximum(best, cs_rx[src])

    prior_row = jnp.broadcast_to(prior_ref[...], (parts, parts))
    prior_col = jnp.sum(jnp.where(eye, prior_row, 0), axis=1, keepdims=True)
    chosen = (prior_col == lane + cls * classes) & (lane < classes)
    top = jnp.max(best, axis=1, keepdims=True)
    earlier = jnp.max(jnp.where(chosen, best, LOW), axis=1, keepdims=True)
    bp[cls] = jnp.where(lane == 0, top, earlier)

    def bp_copy(d, slot_):
        return pltpu.make_async_remote_copy(
            src_ref=bp.at[slot_], dst_ref=bp.at[slot_], send_sem=bp_send.at[d],
            recv_sem=bp_recv.at[slot_], device_id=(rot, lax.rem(cls + d, n_cls)),
            device_id_type=pl.DeviceIdType.MESH)
    for d in range(1, n_cls):
        bp_copy(d, cls).start()
    both = bp[cls]
    for d in range(1, n_cls):
        src = lax.rem(cls + n_cls - d, n_cls)
        bp_copy(d, src).wait_recv()
        both = jnp.maximum(both, bp[src])
    res_out[...] = jnp.where(lane == 126, both[:, 0:1], jnp.where(lane == 127, both[:, 1:2], best))
    for d in range(1, n_rot):
        score_copy(d, rot, rot).wait_send()
    for d in range(1, n_cls):
        bp_copy(d, cls).wait_send()


def finish(res_ref, cls_out, best_out, prior_out):
    res = res_ref[...]
    parts, classes = cls_out.shape
    cls_out[...] = res[:, :classes]
    eye = (lax.broadcasted_iota(jnp.int32, (parts, parts), 0)
           == lax.broadcasted_iota(jnp.int32, (parts, parts), 1))
    best_out[...] = jnp.max(jnp.where(eye, res[:, 126:127], LOW), axis=0, keepdims=True)
    prior_out[...] = jnp.max(jnp.where(eye, res[:, 127:128], LOW), axis=0, keepdims=True)


def part_value(g, rot, r, step):
    return g[rot, :, r * step:(r + 1) * step].astype(jnp.float32)


def body(n_rot, n_cls, particles, references, micrograph, ctf, prior_class):
    parts, feats = particles.shape
    classes, angles, _ = references.shape
    padded = -(-angles // 16) * 16
    units = len(plan(n_rot, n_cls)[4])
    vmem = pl.BlockSpec(memory_space=pltpu.VMEM)
    hbm = pl.BlockSpec(memory_space=pl.ANY)
    dma = pltpu.SemaphoreType.DMA
    total = n_rot * parts
    res = pl.pallas_call(
        functools.partial(kernel, n_rot, n_cls),
        out_shape=jax.ShapeDtypeStruct((parts, 128), jnp.float32),
        in_specs=[hbm, hbm, vmem, vmem, vmem],
        out_specs=vmem,
        scratch_shapes=[
            pltpu.VMEM((n_rot, parts, feats), jnp.bfloat16),
            pltpu.VMEM((classes, angles, feats), jnp.bfloat16),
            pltpu.VMEM((classes, padded, feats), jnp.bfloat16),
            pltpu.VMEM((classes * padded, total), jnp.float32),
            pltpu.VMEM((n_rot, parts, 128), jnp.float32),
            pltpu.VMEM((128, total), jnp.float32),
            pltpu.VMEM((n_rot, parts, 128), jnp.float32),
            pltpu.VMEM((n_rot, parts, 128), jnp.float32),
            pltpu.VMEM((n_cls, parts, 128), jnp.float32),
            dma, dma((classes,)), dma((n_rot, 2 * units)), dma((5, n_rot, units)),
            dma((3, n_rot)), dma((n_rot,)), dma((n_rot,)), dma((n_rot,)),
            dma((n_cls,)), dma((n_cls,)),
        ],
        compiler_params=pltpu.CompilerParams(
            collective_id=0, has_side_effects=True, vmem_limit_bytes=VMEM_BYTES),
    )(particles, references, micrograph, ctf, prior_class.reshape(1, parts))
    out = pl.pallas_call(
        finish,
        out_shape=(jax.ShapeDtypeStruct((parts, classes), jnp.float32),
                   jax.ShapeDtypeStruct((1, parts), jnp.float32),
                   jax.ShapeDtypeStruct((1, parts), jnp.float32)),
        in_specs=[vmem], out_specs=(vmem, vmem, vmem),
    )(res)
    return out[0], out[1].reshape(parts), out[2].reshape(parts)


def solution(mesh):
    in_specs = (P("rot", None), P("cls", "rot", None), P("rot", None), P("rot", None), P("rot"))
    out_specs = (P("rot", "cls"), P("rot"), P("rot"))
    fn = functools.partial(body, mesh.shape["rot"], mesh.shape["cls"])
    return jax.shard_map(fn, mesh=mesh, in_specs=in_specs, out_specs=out_specs, check_vma=False)
```

```python
import functools
import jax
import jax.numpy as jnp
from jax import lax
from jax.experimental import pallas as pl
from jax.experimental.pallas import tpu as pltpu
from jax.sharding import PartitionSpec as P

CYCLES = 64
LOW = -1e30
EDGE, MIDS = 6, 1
XLAG, YLAG = 2, 3
VMEM_BYTES = 62 * 1024 * 1024


def plan(n_rot, n_cls):
    ys = 2 if n_rot % 2 == 0 else 1
    cs = 2 if n_cls % 2 == 0 else 1
    half = CYCLES // cs
    if n_cls == 2 * cs and n_rot <= 16:
        edge = (EDGE * half) // 32
        mid = half - 4 * edge
        mids = [mid // MIDS] * MIDS
        widths, crossing = [edge, edge] + mids + [edge, edge], 2
    else:
        widths, crossing = [half], 0
    assert sum(widths) == half
    return n_rot // ys, ys, n_cls // cs, cs, widths, crossing


def kernel(n_rot, n_cls, part_ref, ref_ref, mic_ref, ctf_ref, prior_ref,
           res_out,
           g, refs_v, refs_p, acc, fac, fac_t, cs_tx, cs_rx, bp,
           own_sem, ref_sem, recv_sem, send_sem, fac_send, fac_recv,
           sc_send, sc_recv, bp_send, bp_recv):
    zs, ys, xs, cores, widths, crossing = plan(n_rot, n_cls)
    units = len(widths)
    through = units - crossing
    fac_at = min(1, through - 1)
    starts = [sum(widths[:u]) for u in range(units)]
    half_cycles = CYCLES // cores
    parts, feats = part_ref.shape
    classes, angles, _ = ref_ref.shape
    step = feats // CYCLES
    rot = lax.axis_index("rot")
    cls = lax.axis_index("cls")
    z, y = lax.div(rot, ys), lax.rem(rot, ys)
    x, core = lax.div(cls, cores), lax.rem(cls, cores)

    own = pltpu.make_async_copy(part_ref, g.at[rot], own_sem)
    own.start()
    ref_copies = [
        pltpu.make_async_copy(ref_ref.at[c], refs_v.at[c], ref_sem.at[c]) for c in range(classes)
    ]

    up, down = ((z + 1) * ys + y, cls), ((z - 1) * ys + y, cls)
    across = (z * ys + (ys - 1 - y), cls)
    other_x = (rot, (xs - 1 - x) * cores + core)
    mate = (rot, x * cores + (cores - 1 - core))
    has_up, has_down = z + 1 < zs, z >= 1
    at_end = (z == 0) | (z == zs - 1)
    UP, DOWN, ACROSS, OTHER, MATE = range(5)

    barrier = pltpu.get_barrier_semaphore()

    def greet(dev):
        pl.semaphore_signal(barrier, inc=1, device_id=dev,
                            device_id_type=pl.DeviceIdType.MESH)
    near = ([across] if ys == 2 else []) + ([other_x] if crossing else [])
    near += [mate] if cores == 2 else []
    pl.when(has_up)(lambda: greet(up))
    pl.when(has_down)(lambda: greet(down))
    for dev in near:
        greet(dev)
    for copy in ref_copies:
        copy.start()
    pl.semaphore_wait(
        barrier, len(near) + jnp.where(has_up, 1, 0) + jnp.where(has_down, 1, 0))

    def unit_of(j):
        return jnp.where(x == 0, j, units - 1 - j) if crossing else j

    def cycle_of(j, half):
        first_cycle = jnp.where(x == 0, starts[j], starts[units - 1 - j]) if crossing else starts[j]
        return half * half_cycles + first_cycle

    def piece(shard, j, half, dev, kind):
        col = pl.multiple_of(cycle_of(j, half) * step, step)
        ref = g.at[shard, :, pl.ds(col, widths[j] * step)]
        unit = unit_of(j)
        return pltpu.make_async_remote_copy(
            src_ref=ref, dst_ref=ref,
            send_sem=send_sem.at[kind, shard, unit],
            recv_sem=recv_sem.at[shard, half * units + unit],
            device_id=dev, device_id_type=pl.DeviceIdType.MESH)

    def fac_copy(shard, dev, kind):
        return pltpu.make_async_remote_copy(
            src_ref=fac.at[shard], dst_ref=fac.at[shard], send_sem=fac_send.at[kind, shard],
            recv_sem=fac_recv.at[shard], device_id=dev, device_id_type=pl.DeviceIdType.MESH)

    def send(shard, j, dev, kind):
        piece(shard, j, core, dev, kind).start()

    def sent(shard, j, dev, kind):
        piece(shard, j, core, dev, kind).wait_send()

    def send_fac(shard, dev, kind):
        fac_copy(shard, dev, kind).start()

    def sent_fac(shard, dev, kind):
        fac_copy(shard, dev, kind).wait_send()

    def to_chip(act, shard, j):
        if j < crossing:
            act(shard, j, other_x, OTHER)
        if cores == 2:
            act(shard, j, mate, MATE)

    def arrive(shard, j, half):
        piece(shard, j, half, mate, MATE).wait_recv()

    def z_visit(d, j, sign, act, wait):
        shard = (z - sign * d) * ys + y
        exists = (z >= d) if sign > 0 else (z + d < zs)

        def visit():
            if wait:
                arrive(shard, j, core)
            more, dev, kind = (has_up, up, UP) if sign > 0 else (has_down, down, DOWN)
            if d < zs - 1:
                pl.when(more)(lambda: act(shard, j, dev, kind))
            if ys == 2:
                act(shard, j, across, ACROSS)
            to_chip(act, shard, j)
            if j == fac_at:
                if wait:
                    fac_copy(shard, mate, 0).wait_recv()
                fac_act = send_fac if wait else sent_fac
                if d < zs - 1:
                    pl.when(more)(lambda: fac_act(shard, dev, kind))
                if ys == 2:
                    fac_act(shard, across, ACROSS)
        pl.when(exists)(visit)

    def y_visit(d, j, sign, act, wait, where):
        shard = (z - sign * d) * ys + (ys - 1 - y)

        def visit():
            if wait:
                arrive(shard, j, core)
            to_chip(act, shard, j)
            if j == fac_at and wait:
                fac_copy(shard, mate, 0).wait_recv()
        if d == 0:
            visit()
        else:
            pl.when(((z >= d) if sign > 0 else (z + d < zs)) & where)(visit)

    def x_visit(d, j, sign, row, act, wait):
        shard = (z - sign * d) * ys + row
        far = units - 1 - j

        def visit():
            if wait:
                arrive(shard, far, core)
            if cores == 2:
                act(shard, far, mate, MATE)
        if d == 0:
            visit()
        else:
            pl.when((z >= d) if sign > 0 else (z + d < zs))(visit)

    def first(act_on):
        pl.when(has_up)(lambda: act_on(up, UP))
        pl.when(has_down)(lambda: act_on(down, DOWN))
        if ys == 2:
            act_on(across, ACROSS)

    def slot(r, j, act, wait):
        signs = (1, -1)
        if r == 0:
            first(lambda dev, kind: act(rot, j, dev, kind))
        if 1 <= r <= zs - 1:
            for sign in signs:
                z_visit(r, j, sign, act, wait)
        if ys == 2:
            for d in range(zs):
                for sign in (signs if d else (1,)):
                    if r == d + 1:
                        y_visit(d, j, sign, act, wait, at_end if d else None)
                    if r == d + 2 and 1 <= d <= zs - 2:
                        y_visit(d, j, sign, act, wait, jnp.logical_not(at_end))
        if j < crossing:
            for d in range(zs):
                for sign in (signs if d else (1,)):
                    if d and r == d + XLAG:
                        x_visit(d, j, sign, y, act, wait)
                    if ys == 2 and r == min(d + YLAG, zs + 1):
                        x_visit(d, j, sign, ys - 1 - y, act, wait)

    own.wait()
    for j in range(min(2, through)):
        slot(0, j, send, True)

    lane = lax.broadcasted_iota(jnp.int32, (parts, 128), 1)
    power = jnp.zeros((parts, 128), jnp.float32)
    for r in range(CYCLES):
        v = part_value(g, rot, r, step)
        power = jnp.where(lane == r, jnp.sum(v * v, axis=1, keepdims=True) / step, power)
    power = power[:, :CYCLES]
    eye = (lax.broadcasted_iota(jnp.int32, (parts, parts), 0)
           == lax.broadcasted_iota(jnp.int32, (parts, parts), 1))
    mic_row = jnp.broadcast_to(mic_ref[...].astype(jnp.float32), (parts, parts))
    mic_col = jnp.sum(jnp.where(eye, mic_row, 0.0), axis=1, keepdims=True)
    same = (mic_row == mic_col).astype(jnp.float32)
    mean = jnp.dot(same, power, precision=lax.Precision.HIGHEST,
                   preferred_element_type=jnp.float32)
    mean = mean / jnp.sum(same, axis=1, keepdims=True)
    ctf = ctf_ref[...]
    ctf_part = jnp.zeros((parts, CYCLES), jnp.float32)
    for m in range(ctf.shape[0]):
        ctf_part = jnp.where(mic_col == float(m), ctf[m:m + 1, :], ctf_part)
    factor = ctf_part * lax.rsqrt(mean + 1e-6)
    fac[rot] = jnp.concatenate([factor, jnp.zeros((parts, 128 - CYCLES), jnp.float32)], axis=1)
    acc[...] = jnp.zeros_like(acc)
    for j in range(min(2, through), fac_at + 1):
        slot(0, j, send, True)
    first(lambda dev, kind: send_fac(rot, dev, kind))
    for j in range(fac_at + 1, through):
        slot(0, j, send, True)

    for copy in ref_copies:
        copy.wait()

    def pad_block(i, carry):
        cols = pl.ds(pl.multiple_of(i * 1024, 1024), 1024)
        for c in range(classes):
            refs_p[c, 0:angles, cols] = refs_v[c, :, cols]
        return carry
    lax.fori_loop(0, feats // 1024, pad_block, 0)

    for r in range(1, zs):
        for j in range(through):
            slot(r, j, send, True)

    total = n_rot * parts
    rows = refs_p.shape[0] * refs_p.shape[1]

    def cycles_dot(first_cycle, count):
        part_sum = None
        for k in range(count):
            r = first_cycle + k
            cols = pl.ds(pl.multiple_of(r * step, step), step)
            dot = lax.dot_general(
                refs_p[:, :, cols].reshape(rows, step), g[:, :, cols].reshape(total, step),
                (((1,), (1,)), ((), ())), preferred_element_type=jnp.float32)
            dot = dot * fac_t[pl.ds(r, 1), :]
            part_sum = dot if part_sum is None else part_sum + dot
        acc[...] += part_sum

    def compute(j, half):
        if widths[j] <= 8:
            cycles_dot(cycle_of(j, half), widths[j])
        else:
            lax.fori_loop(
                0, widths[j], lambda i, c: (cycles_dot(cycle_of(j, half) + i, 1), c)[1], 0)

    def mate_units(j):
        for d in range(1, n_rot):
            arrive(lax.rem(rot + d, n_rot), j, 1 - core)
        compute(j, 1 - core)

    for j in range(fac_at + 1):
        slot(zs, j, send, True)
    fac_t[...] = fac[...].reshape(total, 128).T
    early = fac_at + 1 if through > fac_at + 1 else 0
    for j in range(early):
        compute(j, core)
    if cores == 2 and early:
        mate_units(0)
    for j in range(fac_at + 1, through):
        slot(zs, j, send, True)
    for j in range(crossing):
        slot(zs + 1, j, send, True)
    if cores == 2:
        for j in range(min(early, 1), early):
            mate_units(j)
    for j in list(range(early, through)) + [units - 1 - j for j in range(crossing)]:
        compute(j, core)
    if cores == 2:
        for j in range(early, units):
            mate_units(j)

    score = acc[...].reshape(classes, refs_p.shape[1], total)
    angle = lax.broadcasted_iota(jnp.int32, score.shape, 1)
    local = jnp.max(jnp.where(angle < angles, score, LOW), axis=1)
    local = jnp.concatenate([local, jnp.full((128 - classes, total), LOW, jnp.float32)], axis=0)
    cs_tx[...] = local.T.reshape(n_rot, parts, 128)

    def score_copy(d, block, slot_):
        return pltpu.make_async_remote_copy(
            src_ref=cs_tx.at[block], dst_ref=cs_rx.at[slot_], send_sem=sc_send.at[d],
            recv_sem=sc_recv.at[slot_], device_id=(lax.rem(rot + d, n_rot), cls),
            device_id_type=pl.DeviceIdType.MESH)
    for d in range(1, n_rot):
        score_copy(d, lax.rem(rot + d, n_rot), rot).start()
    for r in range(zs + 2):
        for j in range(through):
            slot(r, j, sent, False)
    first(lambda dev, kind: sent_fac(rot, dev, kind))
    best = cs_tx[rot]
    for d in range(1, n_rot):
        src = lax.rem(rot + n_rot - d, n_rot)
        score_copy(d, rot, src).wait_recv()
        best = jnp.maximum(best, cs_rx[src])

    prior_row = jnp.broadcast_to(prior_ref[...], (parts, parts))
    prior_col = jnp.sum(jnp.where(eye, prior_row, 0), axis=1, keepdims=True)
    chosen = (prior_col == lane + cls * classes) & (lane < classes)
    top = jnp.max(best, axis=1, keepdims=True)
    earlier = jnp.max(jnp.where(chosen, best, LOW), axis=1, keepdims=True)
    bp[cls] = jnp.where(lane == 0, top, earlier)

    def bp_copy(d, slot_):
        return pltpu.make_async_remote_copy(
            src_ref=bp.at[slot_], dst_ref=bp.at[slot_], send_sem=bp_send.at[d],
            recv_sem=bp_recv.at[slot_], device_id=(rot, lax.rem(cls + d, n_cls)),
            device_id_type=pl.DeviceIdType.MESH)
    for d in range(1, n_cls):
        bp_copy(d, cls).start()
    both = bp[cls]
    for d in range(1, n_cls):
        src = lax.rem(cls + n_cls - d, n_cls)
        bp_copy(d, src).wait_recv()
        both = jnp.maximum(both, bp[src])
    res_out[...] = jnp.where(lane == 126, both[:, 0:1], jnp.where(lane == 127, both[:, 1:2], best))
    for d in range(1, n_rot):
        score_copy(d, rot, rot).wait_send()
    for d in range(1, n_cls):
        bp_copy(d, cls).wait_send()


def finish(res_ref, cls_out, best_out, prior_out):
    res = res_ref[...]
    parts, classes = cls_out.shape
    cls_out[...] = res[:, :classes]
    eye = (lax.broadcasted_iota(jnp.int32, (parts, parts), 0)
           == lax.broadcasted_iota(jnp.int32, (parts, parts), 1))
    best_out[...] = jnp.max(jnp.where(eye, res[:, 126:127], LOW), axis=0, keepdims=True)
    prior_out[...] = jnp.max(jnp.where(eye, res[:, 127:128], LOW), axis=0, keepdims=True)


def part_value(g, rot, r, step):
    return g[rot, :, r * step:(r + 1) * step].astype(jnp.float32)


def body(n_rot, n_cls, particles, references, micrograph, ctf, prior_class):
    parts, feats = particles.shape
    classes, angles, _ = references.shape
    padded = -(-angles // 16) * 16
    units = len(plan(n_rot, n_cls)[4])
    vmem = pl.BlockSpec(memory_space=pltpu.VMEM)
    hbm = pl.BlockSpec(memory_space=pl.ANY)
    dma = pltpu.SemaphoreType.DMA
    total = n_rot * parts
    res = pl.pallas_call(
        functools.partial(kernel, n_rot, n_cls),
        out_shape=jax.ShapeDtypeStruct((parts, 128), jnp.float32),
        in_specs=[hbm, hbm, vmem, vmem, vmem],
        out_specs=vmem,
        scratch_shapes=[
            pltpu.VMEM((n_rot, parts, feats), jnp.bfloat16),
            pltpu.VMEM((classes, angles, feats), jnp.bfloat16),
            pltpu.VMEM((classes, padded, feats), jnp.bfloat16),
            pltpu.VMEM((classes * padded, total), jnp.float32),
            pltpu.VMEM((n_rot, parts, 128), jnp.float32),
            pltpu.VMEM((128, total), jnp.float32),
            pltpu.VMEM((n_rot, parts, 128), jnp.float32),
            pltpu.VMEM((n_rot, parts, 128), jnp.float32),
            pltpu.VMEM((n_cls, parts, 128), jnp.float32),
            dma, dma((classes,)), dma((n_rot, 2 * units)), dma((5, n_rot, units)),
            dma((3, n_rot)), dma((n_rot,)), dma((n_rot,)), dma((n_rot,)),
            dma((n_cls,)), dma((n_cls,)),
        ],
        compiler_params=pltpu.CompilerParams(
            collective_id=0, has_side_effects=True, vmem_limit_bytes=VMEM_BYTES),
    )(particles, references, micrograph, ctf, prior_class.reshape(1, parts))
    out = pl.pallas_call(
        finish,
        out_shape=(jax.ShapeDtypeStruct((parts, classes), jnp.float32),
                   jax.ShapeDtypeStruct((1, parts), jnp.float32),
                   jax.ShapeDtypeStruct((1, parts), jnp.float32)),
        in_specs=[vmem], out_specs=(vmem, vmem, vmem),
    )(res)
    return out[0], out[1].reshape(parts), out[2].reshape(parts)


def solution(mesh):
    in_specs = (P("rot", None), P("cls", "rot", None), P("rot", None), P("rot", None), P("rot"))
    out_specs = (P("rot", "cls"), P("rot"), P("rot"))
    fn = functools.partial(body, mesh.shape["rot"], mesh.shape["cls"])
    return jax.shard_map(fn, mesh=mesh, in_specs=in_specs, out_specs=out_specs, check_vma=False)
```
